128 devices in a mesh: rows: 2 (over core), cols: 8 (over z, x_lo), slabs: 8 (over y, x_hi).
Axes of the slice: x: 4 (x_hi: 2, x_lo: 2; x = x_hi * 2 + x_lo), y: 4, z: 4, core: 2. Of those that a mesh axis runs over, the one named last changes fastest.
Arguments:
- density: float32 [32, 768, 64, 128], P('rows', 'cols', 'slabs'), may hold values from 0.5 to 2
- flow_j: float32 [32, 768, 64, 128], P('rows', 'cols', 'slabs'), may hold values from -0.3 to 0.3
- flow_i: float32 [32, 768, 64, 128], P('rows', 'cols', 'slabs'), may hold values from -0.3 to 0.3
- flow_k: float32 [32, 768, 64, 128], P('rows', 'cols', 'slabs'), may hold values from -0.3 to 0.3
Outputs:
- anomaly: float32 [32, 768, 64, 128], P('rows', 'cols', 'slabs')
- density_end: float32 [32, 768, 64, 128], P('rows', 'cols', 'slabs')
The draws below stay inside these ranges and needn't reach their ends.
All inputs are finite; a program needn't handle non-finite values.
Results may differ from the reference program's by a relative error of at most 0.00002.
Values sent between devices are 32-bit elements; how exact they have to be, the bound alone decides.
No kernel may reach another device: no remote copies, remote signals or barrier semaphores. Data moves between devices by JAX's collectives and lax.ppermute only.
A program may use at most 128 MiB of HBM per device.

```python
import jax
import jax.numpy as jnp
from jax import lax

GRID_J = 32
GRID_I = 768
GRID_K = 64
LEVELS = 128
STEPS = 6


def block_scale(own_key, extent, shards, least, top_value):
    def one(dim, shards_of):
        steps = jax.random.uniform(jax.random.fold_in(jax.random.fold_in(own_key, 6), dim), (shards_of,), jnp.float32, least / len(shards), top_value / len(shards))
        return jnp.repeat(jnp.exp(steps), extent[dim] // shards_of).reshape((-1,) + (1,) * (len(extent) - dim - 1))

    factor_of = one(*shards[0])
    for cut in shards[1:]:
        factor_of = factor_of * one(*cut)
    return factor_of


def setup_inputs(seed: int = 0) -> dict:
    key_of = jax.random.split(jax.random.key(seed), 5)
    density = jnp.clip(0.5 + 1.5 * jax.random.uniform(key_of[0], (GRID_J, GRID_I, GRID_K, LEVELS), jnp.float32) ** block_scale(key_of[0], (GRID_J, GRID_I, GRID_K, LEVELS), ((0, 2), (1, 8), (2, 8)), -0.2, 0.2), 0.5, 2.0)
    flow_j = jnp.clip(jax.random.uniform(key_of[1], (GRID_J, GRID_I, GRID_K, LEVELS), jnp.float32, -0.3, 0.3) * block_scale(key_of[1], (GRID_J, GRID_I, GRID_K, LEVELS), ((0, 2), (1, 8), (2, 8)), -0.4, 0.0), -0.3, 0.3)
    flow_i = jnp.clip(jax.random.uniform(key_of[2], (GRID_J, GRID_I, GRID_K, LEVELS), jnp.float32, -0.3, 0.3) * block_scale(key_of[2], (GRID_J, GRID_I, GRID_K, LEVELS), ((0, 2), (1, 8), (2, 8)), -0.4, 0.0), -0.3, 0.3)
    flow_k = jnp.clip(jax.random.uniform(key_of[3], (GRID_J, GRID_I, GRID_K, LEVELS), jnp.float32, -0.3, 0.3) * block_scale(key_of[3], (GRID_J, GRID_I, GRID_K, LEVELS), ((0, 2), (1, 8), (2, 8)), -0.4, 0.0), -0.3, 0.3)
    return {"density": density, "flow_j": flow_j, "flow_i": flow_i, "flow_k": flow_k}


def inner_cells(values, dims):
    for dim in dims:
        values = lax.slice_in_dim(values, 1, values.shape[dim] - 1, axis=dim)
    return values

def side_cells(values, dim, start, dims):
    others = [other for other in dims if other != dim]
    values = inner_cells(values, others)
    return lax.slice_in_dim(values, start, start + values.shape[dim] - 2, axis=dim)

def advance(padded, flow_j, flow_i, flow_k):
    middle = inner_cells(padded, (0, 1, 2))
    lower = [side_cells(padded, dim, 0, (0, 1, 2)) for dim in (0, 1, 2)]
    upper = [side_cells(padded, dim, 2, (0, 1, 2)) for dim in (0, 1, 2)]
    slopes = [above - below for above, below in zip(upper, lower)]
    smooth_rate = 0.05
    spread = lower[0] + upper[0] + lower[1] + upper[1] + lower[2] + upper[2] - 6.0 * middle
    return middle - flow_j * slopes[0] - flow_i * slopes[1] - flow_k * slopes[2] + smooth_rate * spread

def reference(density, flow_j, flow_i, flow_k):
    for step in range(STEPS):
        density = advance(jnp.pad(density, ((1, 1), (1, 1), (1, 1), (0, 0)), mode='constant'), flow_j, flow_i, flow_k)
    line_mean = lax.optimization_barrier(jnp.mean(density, axis=2, keepdims=True))
    centred = density - line_mean
    line_variance = lax.optimization_barrier(jnp.mean(centred * centred, axis=2, keepdims=True))
    anomaly = centred * lax.rsqrt(line_variance + 0.0001)
    return (anomaly, density)
```

```python
import functools

import jax
import jax.numpy as jnp
from jax import lax
from jax.experimental import pallas as pl
from jax.experimental.pallas import tpu as pltpu
from jax.sharding import PartitionSpec as P

STEPS = 6
RATE = 0.05
SUB = 8


def step_body(core_ref, d_ref, a0_ref, a7_ref, h_ref, row_ref, lo_ref, hi_ref, fj_ref, fi_ref, fk_ref, *rest, nj, ni, first, last):
    if last:
        out_ref, af_ref, ps_ref, mid_ref, s1_ref, s2_ref, ring = rest
    else:
        out_ref, af_ref, ps_ref, ring = rest
    rows = ni * SUB
    pitch = rows + 2 * SUB
    other = 7 - first
    g = pl.program_id(0)
    core = core_ref[0]
    here = lax.rem(g, 3) * pitch
    middle = lax.rem(g + 2, 3) * pitch
    below = lax.rem(g + 1, 3) * pitch

    @pl.when(g == 0)
    def _():
        ring[pl.ds(middle + SUB, rows), :] = jnp.where(core == 1, row_ref[...], 0.0)

    @pl.when(g < nj)
    def _():
        ring[pl.ds(here + SUB, rows), :] = d_ref[0]
        ring[pl.ds(here + SUB, ni, stride=SUB), :] = a0_ref[0]
        ring[pl.ds(here + SUB + 7, ni, stride=SUB), :] = a7_ref[0]
        ring[pl.ds(here, SUB), :] = lo_ref[0]
        ring[pl.ds(here + SUB + rows, SUB), :] = hi_ref[0]

    @pl.when(g == nj)
    def _():
        ring[pl.ds(here + SUB, rows), :] = jnp.where(core == 0, row_ref[...], 0.0)

    @pl.when(g > 0)
    def _():
        level = lax.broadcasted_iota(jnp.int32, (SUB, 128), 0)
        unroll = 8

        def some(n, carry):
            base = pl.multiple_of(n * (unroll * SUB), SUB)
            for m in range(unroll):
                at = base + m * SUB
                mid = pl.multiple_of(middle + SUB + at, SUB)
                c = ring[pl.ds(mid, SUB), :]
                i_lo = ring[pl.ds(mid - SUB, SUB), :]
                i_hi = ring[pl.ds(mid + SUB, SUB), :]
                j_lo = ring[pl.ds(pl.multiple_of(below + SUB + at, SUB), SUB), :]
                j_hi = ring[pl.ds(pl.multiple_of(here + SUB + at, SUB), SUB), :]
                k_lo = jnp.where(level == 0, 0.0, pltpu.roll(c, 1, 0))
                k_hi = jnp.where(level == 7, 0.0, pltpu.roll(c, 7, 0))
                total = (j_lo + j_hi) + (i_lo + i_hi) + (k_lo + k_hi)
                new = (1.0 - 6.0 * RATE) * c + RATE * total
                new = new - fj_ref[0, pl.ds(at, SUB), :] * (j_hi - j_lo)
                new = new - fi_ref[0, pl.ds(at, SUB), :] * (i_hi - i_lo)
                new = new - fk_ref[0, pl.ds(at, SUB), :] * (k_hi - k_lo)
                out_ref[0, pl.ds(at, SUB), :] = new
            return carry

        lax.fori_loop(0, ni // unroll, some, 0)
        flow = fk_ref[0, pl.ds(first, ni, stride=SUB), :]
        gain = RATE + flow if first == 0 else RATE - flow
        exact = out_ref[0, pl.ds(first, ni, stride=SUB), :] + gain * h_ref[0]
        af_ref[0] = exact
        ps_ref[0] = out_ref[0, pl.ds(other, ni, stride=SUB), :]
        if last:
            centre = out_ref[0, pl.ds(3, ni, stride=SUB), :]
            moved = exact - centre
            s1 = moved
            s2 = moved * moved
            for k in (1, 2, 4, 5, 6):
                moved = out_ref[0, pl.ds(k, ni, stride=SUB), :] - centre
                s1 = s1 + moved
                s2 = s2 + moved * moved
            mid_ref[0] = centre
            s1_ref[0] = s1
            s2_ref[0] = s2


def step_call(core, d, a0, a7, h, row, lo, hi, fj, fi, fk, first, last):
    nj, rows, lanes = d.shape
    ni = rows // SUB
    ahead = lambda g, *_: (jnp.minimum(g, nj - 1), 0, 0)
    behind = lambda g, *_: (jnp.maximum(g - 1, 0), 0, 0)
    block = lambda n, at: pl.BlockSpec((1, n, lanes), at)
    plane = jax.ShapeDtypeStruct((nj, ni, lanes), d.dtype)
    extra = 3 if last else 0
    return pl.pallas_call(
        functools.partial(step_body, nj=nj, ni=ni, first=first, last=last),
        grid_spec=pltpu.PrefetchScalarGridSpec(
            num_scalar_prefetch=1,
            grid=(nj + 1,),
            in_specs=[
                block(rows, ahead),
                block(ni, ahead),
                block(ni, ahead),
                block(ni, behind),
                pl.BlockSpec((rows, lanes), lambda g, *_: (0, 0)),
                block(SUB, ahead),
                block(SUB, ahead),
                block(rows, behind),
                block(rows, behind),
                block(rows, behind),
            ],
            out_specs=[block(rows, behind)] + [block(ni, behind)] * (2 + extra),
            scratch_shapes=[pltpu.VMEM((3 * (rows + 2 * SUB), lanes), jnp.float32)],
        ),
        out_shape=[jax.ShapeDtypeStruct(d.shape, d.dtype)] + [plane] * (2 + extra),
    )(core, d, a0, a7, h, row, lo, hi, fj, fi, fk)


def fix_body(core_ref, ps_ref, g_ref, h_ref, af_ref, row_ref, lo_ref, hi_ref, as_ref, row_out, lo_out, hi_out, *, ni, nj, first):
    other = 7 - first
    as_ref[...] = ps_ref[...] + g_ref[...] * h_ref[...]
    edge = (1 - core_ref[0]) * (nj - 1)
    row_out[...] = row_ref[0]
    row_out[pl.ds(first, ni, stride=SUB), :] = af_ref[edge]
    row_out[pl.ds(other, ni, stride=SUB), :] = as_ref[edge]
    level = lax.broadcasted_iota(jnp.int32, (SUB, 128), 0)
    for j in range(nj):
        for src, dst, i in ((lo_ref, lo_out, 0), (hi_ref, hi_out, ni - 1)):
            v = jnp.where(level == first, af_ref[j, pl.ds(i, 1), :], src[j])
            dst[j] = jnp.where(level == other, as_ref[j, pl.ds(i, 1), :], v)


def fix_call(core, ps, g, h, af, d, first):
    nj, rows, lanes = d.shape
    ni = rows // SUB
    whole = pl.BlockSpec((nj, ni, lanes), lambda g, c: (0, 0, 0))
    return pl.pallas_call(
        functools.partial(fix_body, ni=ni, nj=nj, first=first),
        grid_spec=pltpu.PrefetchScalarGridSpec(
            num_scalar_prefetch=1,
            grid=(1,),
            in_specs=[
                whole,
                whole,
                whole,
                whole,
                pl.BlockSpec((1, rows, lanes), lambda g, c: ((1 - c[0]) * (nj - 1), 0, 0)),
                pl.BlockSpec((nj, SUB, lanes), lambda g, c: (0, 0, 0)),
                pl.BlockSpec((nj, SUB, lanes), lambda g, c: (0, ni - 1, 0)),
            ],
            out_specs=[
                whole,
                pl.BlockSpec((rows, lanes), lambda g, c: (0, 0)),
                pl.BlockSpec((nj, SUB, lanes), lambda g, c: (0, 0, 0)),
                pl.BlockSpec((nj, SUB, lanes), lambda g, c: (0, 0, 0)),
            ],
        ),
        out_shape=[
            jax.ShapeDtypeStruct((nj, ni, lanes), d.dtype),
            jax.ShapeDtypeStruct((rows, lanes), d.dtype),
            jax.ShapeDtypeStruct((nj, SUB, lanes), d.dtype),
            jax.ShapeDtypeStruct((nj, SUB, lanes), d.dtype),
        ],
    )(core, ps, g, h, af, d, d, d)


def sums_body(ps_ref, g_ref, h_ref, mid_ref, s1_ref, s2_ref, as_ref, v_ref):
    exact = ps_ref[...] + g_ref[...] * h_ref[...]
    as_ref[...] = exact
    moved = exact - mid_ref[...]
    s1 = s1_ref[...] + moved
    s2 = s2_ref[...] + moved * moved
    v_ref[:, 0] = mid_ref[...] + s1 * (1.0 / SUB)
    v_ref[:, 1] = s2 - s1 * s1 * (1.0 / SUB)


def sums_call(ps, g, h, mid, s1, s2):
    nj, ni, lanes = ps.shape
    tile = 2
    block = pl.BlockSpec((tile, ni, lanes), lambda n: (n, 0, 0))
    return pl.pallas_call(
        sums_body,
        grid=(nj // tile,),
        in_specs=[block] * 6,
        out_specs=[block, pl.BlockSpec((tile, 2, ni, lanes), lambda n: (n, 0, 0, 0))],
        out_shape=[jax.ShapeDtypeStruct(ps.shape, ps.dtype), jax.ShapeDtypeStruct((nj, 2, ni, lanes), ps.dtype)],
        name="sums",
    )(ps, g, h, mid, s1, s2)


def finish_body(d_ref, a0_ref, a7_ref, v_ref, anomaly_ref, end_ref, *, ni):
    end_ref[0] = d_ref[0]
    end_ref[0, pl.ds(0, ni, stride=SUB), :] = a0_ref[0]
    end_ref[0, pl.ds(7, ni, stride=SUB), :] = a7_ref[0]
    unroll = 8

    def some(n, carry):
        for m in range(unroll):
            i = n * unroll + m
            at = pl.multiple_of(i * SUB, SUB)
            mean = v_ref[0, 0, pl.ds(i, 1), :]
            scale = v_ref[0, 1, pl.ds(i, 1), :]
            anomaly_ref[0, pl.ds(at, SUB), :] = (end_ref[0, pl.ds(at, SUB), :] - mean) * scale
        return carry

    lax.fori_loop(0, ni // unroll, some, 0)


def finish_call(d, a0, a7, v):
    nj, rows, lanes = d.shape
    ni = rows // SUB
    block = lambda n: pl.BlockSpec((1, n, lanes), lambda j: (j, 0, 0))
    return pl.pallas_call(
        functools.partial(finish_body, ni=ni),
        grid=(nj,),
        in_specs=[block(rows), block(ni), block(ni), pl.BlockSpec((1, 2, ni, lanes), lambda j: (j, 0, 0, 0))],
        out_specs=[block(rows), block(rows)],
        out_shape=[jax.ShapeDtypeStruct(d.shape, d.dtype)] * 2,
        name="finish",
    )(d, a0, a7, v)


def send(value, axis, direction):
    size = lax.axis_size(axis)
    up = [(i, i + 1) for i in range(size - 1)]
    return lax.ppermute(value, axis, up if direction > 0 else [(b, a) for a, b in up])


def body(density, flow_j, flow_i, flow_k):
    nj, ni, nk, lanes = density.shape
    flat = lambda v: v.reshape(nj, ni * nk, lanes)
    core = lax.axis_index("rows").astype(jnp.int32).reshape(1)
    slabs = lax.axis_size("slabs")
    d, fj, fi, fk = flat(density), flat(flow_j), flat(flow_i), flat(flow_k)
    planes = {0: density[:, :, 0, :], 7: density[:, :, 7, :]}
    gains = {0: RATE + flow_k[:, :, 0, :], 7: RATE - flow_k[:, :, 7, :]}
    edge = (1 - core[0]) * (nj - 1)
    row_send = lax.dynamic_index_in_dim(d, edge, 0, keepdims=False)
    lo_send = density[:, 0]
    hi_send = density[:, ni - 1]
    halo = {}
    for t in range(STEPS):
        first = 7 if t % 2 == 0 else 0
        other = 7 - first
        if t == 0:
            halo[first] = send(planes[other], "slabs", -1 if other == 0 else 1)
        row = lax.ppermute(row_send, "rows", [(0, 1), (1, 0)])
        hi = send(lo_send, "cols", -1)
        lo = send(hi_send, "cols", 1)
        halo[other] = send(planes[first], "slabs", -1 if first == 0 else 1)
        last = t == STEPS - 1
        d, exact, part, *sums = step_call(
            core, d, planes[0], planes[7], halo[first], row, lo, hi, fj, fi, fk, first, last
        )
        if last:
            break
        early = send(exact, "slabs", -1 if first == 0 else 1)
        fixed, row_send, lo_send, hi_send = fix_call(core, part, gains[other], halo[other], exact, d, first)
        planes = {first: exact, other: fixed}
        halo = {other: early}
    fixed, v = sums_call(part, gains[other], halo[other], *sums)
    planes = {first: exact, other: fixed}
    got = lax.all_to_all(v, "slabs", 0, 0, tiled=True)
    got = got.reshape(slabs, nj // slabs, 2, ni, lanes)
    mean = jnp.sum(got[:, :, 0], axis=0) / slabs
    off = got[:, :, 0] - mean
    line_variance = jnp.sum(got[:, :, 1] + nk * (off * off), axis=0) / (nk * slabs)
    mine = jnp.stack([mean, lax.rsqrt(line_variance + 0.0001)], axis=1)
    v = lax.all_gather(mine, "slabs", axis=0, tiled=True)
    anomaly, end = finish_call(d, planes[0], planes[7], v)
    return (anomaly.reshape(density.shape), end.reshape(density.shape))


def solution(mesh):
    placed = P("rows", "cols", "slabs", None)
    return jax.shard_map(
        body,
        mesh=mesh,
        in_specs=(placed,) * 4,
        out_specs=(placed, placed),
        check_vma=False,
    )
```

```python
import functools

import jax
import jax.numpy as jnp
from jax import lax
from jax.experimental import pallas as pl
from jax.experimental.pallas import tpu as pltpu
from jax.sharding import PartitionSpec as P

STEPS = 6
RATE = 0.05
SUB = 8


def in_vmem(*values):
    return [pltpu.with_memory_space_constraint(v, pltpu.VMEM) for v in values]


def local_call(body, outs, core, *values, scratch=()):
    spec = pl.BlockSpec(memory_space=pltpu.VMEM)
    return pl.pallas_call(
        body,
        in_specs=[pl.BlockSpec(memory_space=pltpu.SMEM)] + [spec] * len(values),
        out_specs=[spec] * len(outs),
        out_shape=[pltpu.VMEM(shape, jnp.float32) for shape in outs],
        scratch_shapes=list(scratch),
        compiler_params=pltpu.CompilerParams(vmem_limit_bytes=4 << 20),
    )(core, *in_vmem(*values))


def prep_body(core_ref, d_ref, a0_ref, a7_ref, row_ref, lo_ref, hi_ref):
    nj, rows, _ = d_ref.shape
    ni = rows // SUB

    def some(j, carry):
        a0_ref[j] = d_ref[j, pl.ds(0, ni, stride=SUB), :]
        a7_ref[j] = d_ref[j, pl.ds(7, ni, stride=SUB), :]
        lo_ref[j] = d_ref[j, pl.ds(0, SUB), :]
        hi_ref[j] = d_ref[j, pl.ds(rows - SUB, SUB), :]
        return carry

    lax.fori_loop(0, nj, some, 0)
    row_ref[...] = d_ref[(1 - core_ref[0]) * (nj - 1)]


def step_body(core_ref, d_ref, a0_ref, a7_ref, h_ref, row_ref, lo_ref, hi_ref, fj_ref, fi_ref, fk_ref, *rest, first, last):
    if last:
        out_ref, af_ref, ps_ref, mid_ref, s1_ref, s2_ref, ring = rest
    else:
        out_ref, af_ref, ps_ref, ring = rest
    nj, rows, _ = d_ref.shape
    ni = rows // SUB
    pitch = rows + 2 * SUB
    other = 7 - first
    core = core_ref[0]
    level = lax.broadcasted_iota(jnp.int32, (SUB, 128), 0)

    def load(j):
        at = pl.multiple_of(lax.rem(j, 3) * pitch, SUB)
        ring[pl.ds(at + SUB, rows), :] = d_ref[j]
        ring[pl.ds(at + SUB, ni, stride=SUB), :] = a0_ref[j]
        ring[pl.ds(at + SUB + 7, ni, stride=SUB), :] = a7_ref[j]
        ring[pl.ds(at, SUB), :] = lo_ref[j]
        ring[pl.ds(at + SUB + rows, SUB), :] = hi_ref[j]

    ring[pl.ds(2 * pitch + SUB, rows), :] = jnp.where(core == 1, row_ref[...], 0.0)
    load(0)

    def plane(j, carry):
        here = lax.rem(j + 1, 3) * pitch
        middle = lax.rem(j, 3) * pitch
        below = lax.rem(j + 2, 3) * pitch

        @pl.when(j + 1 < nj)
        def _():
            load(j + 1)

        @pl.when(j + 1 == nj)
        def _():
            ring[pl.ds(pl.multiple_of(here + SUB, SUB), rows), :] = jnp.where(core == 0, row_ref[...], 0.0)

        unroll = 8

        def some(n, inner):
            base = pl.multiple_of(n * (unroll * SUB), SUB)
            for m in range(unroll):
                at = base + m * SUB
                mid = pl.multiple_of(middle + SUB + at, SUB)
                c = ring[pl.ds(mid, SUB), :]
                i_lo = ring[pl.ds(mid - SUB, SUB), :]
                i_hi = ring[pl.ds(mid + SUB, SUB), :]
                j_lo = ring[pl.ds(pl.multiple_of(below + SUB + at, SUB), SUB), :]
                j_hi = ring[pl.ds(pl.multiple_of(here + SUB + at, SUB), SUB), :]
                k_lo = jnp.where(level == 0, 0.0, pltpu.roll(c, 1, 0))
                k_hi = jnp.where(level == 7, 0.0, pltpu.roll(c, 7, 0))
                total = (j_lo + j_hi) + (i_lo + i_hi) + (k_lo + k_hi)
                new = (1.0 - 6.0 * RATE) * c + RATE * total
                new = new - fj_ref[j, pl.ds(at, SUB), :] * (j_hi - j_lo)
                new = new - fi_ref[j, pl.ds(at, SUB), :] * (i_hi - i_lo)
                new = new - fk_ref[j, pl.ds(at, SUB), :] * (k_hi - k_lo)
                out_ref[j, pl.ds(at, SUB), :] = new
            return inner

        lax.fori_loop(0, ni // unroll, some, 0)
        flow = fk_ref[j, pl.ds(first, ni, stride=SUB), :]
        gain = RATE + flow if first == 0 else RATE - flow
        exact = out_ref[j, pl.ds(first, ni, stride=SUB), :] + gain * h_ref[j]
        af_ref[j] = exact
        ps_ref[j] = out_ref[j, pl.ds(other, ni, stride=SUB), :]
        if last:
            centre = out_ref[j, pl.ds(3, ni, stride=SUB), :]
            moved = exact - centre
            s1 = moved
            s2 = moved * moved
            for k in (1, 2, 4, 5, 6):
                moved = out_ref[j, pl.ds(k, ni, stride=SUB), :] - centre
                s1 = s1 + moved
                s2 = s2 + moved * moved
            mid_ref[j] = centre
            s1_ref[j] = s1
            s2_ref[j] = s2
        return carry

    lax.fori_loop(0, nj, plane, 0)


def fixed_plane(j, ps_ref, h_ref, fk_ref, first):
    ni = ps_ref.shape[1]
    flow = fk_ref[j, pl.ds(7 - first, ni, stride=SUB), :]
    gain = RATE - flow if first == 0 else RATE + flow
    return ps_ref[j] + gain * h_ref[j]


def fix_body(core_ref, ps_ref, fk_ref, h_ref, af_ref, d_ref, as_ref, row_out, lo_out, hi_out, *, first):
    nj, rows, _ = d_ref.shape
    ni = rows // SUB
    other = 7 - first
    level = lax.broadcasted_iota(jnp.int32, (SUB, 128), 0)

    def some(j, carry):
        as_ref[j] = fixed_plane(j, ps_ref, h_ref, fk_ref, first)
        for dst, i in ((lo_out, 0), (hi_out, ni - 1)):
            v = jnp.where(level == first, af_ref[j, pl.ds(i, 1), :], d_ref[j, pl.ds(i * SUB, SUB), :])
            dst[j] = jnp.where(level == other, as_ref[j, pl.ds(i, 1), :], v)
        return carry

    lax.fori_loop(0, nj, some, 0)
    edge = (1 - core_ref[0]) * (nj - 1)
    row_out[...] = d_ref[edge]
    row_out[pl.ds(first, ni, stride=SUB), :] = af_ref[edge]
    row_out[pl.ds(other, ni, stride=SUB), :] = as_ref[edge]


def sums_body(core_ref, ps_ref, fk_ref, h_ref, mid_ref, s1_ref, s2_ref, as_ref, v_ref, *, first):
    def some(j, carry):
        exact = fixed_plane(j, ps_ref, h_ref, fk_ref, first)
        as_ref[j] = exact
        moved = exact - mid_ref[j]
        s1 = s1_ref[j] + moved
        s2 = s2_ref[j] + moved * moved
        v_ref[j, 0] = mid_ref[j] + s1 * (1.0 / SUB)
        v_ref[j, 1] = s2 - s1 * s1 * (1.0 / SUB)
        return carry

    lax.fori_loop(0, ps_ref.shape[0], some, 0)


def finish_body(d_ref, a0_ref, a7_ref, v_ref, anomaly_ref, end_ref):
    j = pl.program_id(0)
    ni = a0_ref.shape[1]
    end_ref[0] = d_ref[j]
    end_ref[0, pl.ds(0, ni, stride=SUB), :] = a0_ref[j]
    end_ref[0, pl.ds(7, ni, stride=SUB), :] = a7_ref[j]
    unroll = 8

    def some(n, carry):
        for m in range(unroll):
            i = n * unroll + m
            at = pl.multiple_of(i * SUB, SUB)
            mean = v_ref[j, 0, pl.ds(i, 1), :]
            scale = v_ref[j, 1, pl.ds(i, 1), :]
            anomaly_ref[0, pl.ds(at, SUB), :] = (end_ref[0, pl.ds(at, SUB), :] - mean) * scale
        return carry

    lax.fori_loop(0, ni // unroll, some, 0)


def finish_call(d, a0, a7, v):
    nj, rows, lanes = d.shape
    whole = pl.BlockSpec(memory_space=pltpu.VMEM)
    block = pl.BlockSpec((1, rows, lanes), lambda j: (j, 0, 0))
    return pl.pallas_call(
        finish_body,
        grid=(nj,),
        in_specs=[whole] * 4,
        out_specs=[block, block],
        out_shape=[jax.ShapeDtypeStruct(d.shape, d.dtype)] * 2,
        compiler_params=pltpu.CompilerParams(vmem_limit_bytes=4 << 20),
        name="finish",
    )(*in_vmem(d, a0, a7, v))


def send(value, axis, direction):
    size = lax.axis_size(axis)
    up = [(i, i + 1) for i in range(size - 1)]
    return lax.ppermute(value, axis, up if direction > 0 else [(b, a) for a, b in up])


def body(density, flow_j, flow_i, flow_k):
    nj, ni, nk, lanes = density.shape
    flat = lambda v: v.reshape(nj, ni * nk, lanes)
    core = lax.axis_index("rows").astype(jnp.int32).reshape(1)
    slabs = lax.axis_size("slabs")
    d, fj, fi, fk = flat(density), flat(flow_j), flat(flow_i), flat(flow_k)
    cube, square, line = d.shape, (nj, ni, lanes), (nj, SUB, lanes)
    edges = [cube[1:], line, line]
    ring = [pltpu.VMEM((3 * (cube[1] + 2 * SUB), lanes), jnp.float32)]
    plane_0, plane_7, row_send, lo_send, hi_send = local_call(
        prep_body, [square, square, *edges], core, d
    )
    planes = {0: plane_0, 7: plane_7}
    halo = {}
    for t in range(STEPS):
        first = 7 if t % 2 == 0 else 0
        other = 7 - first
        last = t == STEPS - 1
        if t == 0:
            halo[first] = send(planes[other], "slabs", -1)
        row = lax.ppermute(row_send, "rows", [(0, 1), (1, 0)])
        hi = send(lo_send, "cols", -1)
        lo = send(hi_send, "cols", 1)
        halo[other] = send(planes[first], "slabs", -1 if first == 0 else 1)
        d, exact, part, *sums = local_call(
            functools.partial(step_body, first=first, last=last),
            [cube] + [square] * (5 if last else 2),
            core,
            *(d, planes[0], planes[7], halo[first], row, lo, hi, fj, fi, fk),
            scratch=ring,
        )
        if last:
            break
        early = send(exact, "slabs", -1 if first == 0 else 1)
        fixed, row_send, lo_send, hi_send = local_call(
            functools.partial(fix_body, first=first),
            [square, *edges],
            core,
            *(part, fk, halo[other], exact, d),
        )
        planes = {first: exact, other: fixed}
        halo = {other: early}
    fixed, v = local_call(
        functools.partial(sums_body, first=first),
        [square, (nj, 2, ni, lanes)],
        core,
        *(part, fk, halo[other], *sums),
    )
    planes = {first: exact, other: fixed}
    got = lax.all_to_all(v, "slabs", 0, 0, tiled=True)
    got = got.reshape(slabs, nj // slabs, 2, ni, lanes)
    mean = jnp.sum(got[:, :, 0], axis=0) / slabs
    off = got[:, :, 0] - mean
    line_variance = jnp.sum(got[:, :, 1] + nk * (off * off), axis=0) / (nk * slabs)
    mine = jnp.stack([mean, lax.rsqrt(line_variance + 0.0001)], axis=1)
    copies = jnp.broadcast_to(mine[None], (slabs, *mine.shape))
    v = lax.all_to_all(copies, "slabs", 0, 0, tiled=True).reshape(nj, 2, ni, lanes)
    anomaly, end = finish_call(d, planes[0], planes[7], v)
    return (anomaly.reshape(density.shape), end.reshape(density.shape))


def solution(mesh):
    placed = P("rows", "cols", "slabs", None)
    return jax.shard_map(
        body,
        mesh=mesh,
        in_specs=(placed,) * 4,
        out_specs=(placed, placed),
        check_vma=False,
    )
```

```python
import functools

import jax
import jax.numpy as jnp
from jax import lax
from jax.experimental import pallas as pl
from jax.experimental.pallas import tpu as pltpu
from jax.sharding import PartitionSpec as P

STEPS = 6
RATE = 0.05
SUB = 8


def in_vmem(*values):
    return [pltpu.with_memory_space_constraint(v, pltpu.VMEM) for v in values]


def local_call(body, outs, core, *values, scratch=(), aliases={}):
    spec = pl.BlockSpec(memory_space=pltpu.VMEM)
    return pl.pallas_call(
        body,
        in_specs=[pl.BlockSpec(memory_space=pltpu.SMEM)] + [spec] * len(values),
        out_specs=[spec] * len(outs),
        out_shape=[pltpu.VMEM(shape, jnp.float32) for shape in outs],
        scratch_shapes=list(scratch),
        input_output_aliases=aliases,
        compiler_params=pltpu.CompilerParams(vmem_limit_bytes=4 << 20),
    )(core, *in_vmem(*values))


def fetch_body(*refs):
    count = len(refs) // 3
    copies = [pltpu.make_async_copy(refs[n], refs[count + n], refs[2 * count + n]) for n in range(count)]
    for copy in copies:
        copy.start()
    for copy in copies:
        copy.wait()


def fetch_call(*values):
    return pl.pallas_call(
        fetch_body,
        in_specs=[pl.BlockSpec(memory_space=pltpu.HBM)] * len(values),
        out_specs=[pl.BlockSpec(memory_space=pltpu.VMEM)] * len(values),
        out_shape=[pltpu.VMEM(v.shape, v.dtype) for v in values],
        scratch_shapes=[pltpu.SemaphoreType.DMA] * len(values),
        compiler_params=pltpu.CompilerParams(vmem_limit_bytes=4 << 20),
        name="fetch",
    )(*[pltpu.with_memory_space_constraint(v, pltpu.HBM) for v in values])


def prep_body(core_ref, d_ref, a0_ref, a7_ref, row_ref, lo_ref, hi_ref):
    nj, rows, _ = d_ref.shape
    ni = rows // SUB

    def some(j, carry):
        a0_ref[j] = d_ref[j, pl.ds(0, ni, stride=SUB), :]
        a7_ref[j] = d_ref[j, pl.ds(7, ni, stride=SUB), :]
        lo_ref[j] = d_ref[j, pl.ds(0, SUB), :]
        hi_ref[j] = d_ref[j, pl.ds(rows - SUB, SUB), :]
        return carry

    lax.fori_loop(0, nj, some, 0)
    row_ref[...] = d_ref[(1 - core_ref[0]) * (nj - 1)]


def step_body(core_ref, d_ref, a0_ref, a7_ref, h_ref, row_ref, lo_ref, hi_ref, fj_ref, fi_ref, fk_ref, *rest, first, last):
    if last:
        out_ref, af_ref, ps_ref, mid_ref, s1_ref, s2_ref, ring = rest
    else:
        out_ref, af_ref, ps_ref, ring = rest
    nj, rows, _ = d_ref.shape
    ni = rows // SUB
    pitch = rows + 2 * SUB
    other = 7 - first
    core = core_ref[0]
    level = lax.broadcasted_iota(jnp.int32, (SUB, 128), 0)

    def load(j):
        at = pl.multiple_of(lax.rem(j, 3) * pitch, SUB)
        ring[pl.ds(at + SUB, rows), :] = d_ref[j]
        ring[pl.ds(at + SUB, ni, stride=SUB), :] = a0_ref[j]
        ring[pl.ds(at + SUB + 7, ni, stride=SUB), :] = a7_ref[j]
        ring[pl.ds(at, SUB), :] = lo_ref[j]
        ring[pl.ds(at + SUB + rows, SUB), :] = hi_ref[j]

    ring[pl.ds(2 * pitch + SUB, rows), :] = jnp.where(core == 1, row_ref[...], 0.0)
    load(0)

    def plane(j, carry):
        here = lax.rem(j + 1, 3) * pitch
        middle = lax.rem(j, 3) * pitch
        below = lax.rem(j + 2, 3) * pitch

        @pl.when(j + 1 < nj)
        def _():
            load(j + 1)

        @pl.when(j + 1 == nj)
        def _():
            ring[pl.ds(pl.multiple_of(here + SUB, SUB), rows), :] = jnp.where(core == 0, row_ref[...], 0.0)

        unroll = 8

        def some(n, inner):
            base = pl.multiple_of(n * (unroll * SUB), SUB)
            for m in range(unroll):
                at = base + m * SUB
                mid = pl.multiple_of(middle + SUB + at, SUB)
                c = ring[pl.ds(mid, SUB), :]
                i_lo = ring[pl.ds(mid - SUB, SUB), :]
                i_hi = ring[pl.ds(mid + SUB, SUB), :]
                j_lo = ring[pl.ds(pl.multiple_of(below + SUB + at, SUB), SUB), :]
                j_hi = ring[pl.ds(pl.multiple_of(here + SUB + at, SUB), SUB), :]
                k_lo = jnp.where(level == 0, 0.0, pltpu.roll(c, 1, 0))
                k_hi = jnp.where(level == 7, 0.0, pltpu.roll(c, 7, 0))
                total = (j_lo + j_hi) + (i_lo + i_hi) + (k_lo + k_hi)
                new = (1.0 - 6.0 * RATE) * c + RATE * total
                new = new - fj_ref[j, pl.ds(at, SUB), :] * (j_hi - j_lo)
                new = new - fi_ref[j, pl.ds(at, SUB), :] * (i_hi - i_lo)
                new = new - fk_ref[j, pl.ds(at, SUB), :] * (k_hi - k_lo)
                out_ref[j, pl.ds(at, SUB), :] = new
            return inner

        lax.fori_loop(0, ni // unroll, some, 0)
        flow = fk_ref[j, pl.ds(first, ni, stride=SUB), :]
        gain = RATE + flow if first == 0 else RATE - flow
        exact = out_ref[j, pl.ds(first, ni, stride=SUB), :] + gain * h_ref[j]
        af_ref[j] = exact
        ps_ref[j] = out_ref[j, pl.ds(other, ni, stride=SUB), :]
        if last:
            out_ref[j, pl.ds(first, ni, stride=SUB), :] = exact
            centre = out_ref[j, pl.ds(3, ni, stride=SUB), :]
            moved = exact - centre
            s1 = moved
            s2 = moved * moved
            for k in (1, 2, 4, 5, 6):
                moved = out_ref[j, pl.ds(k, ni, stride=SUB), :] - centre
                s1 = s1 + moved
                s2 = s2 + moved * moved
            mid_ref[j] = centre
            s1_ref[j] = s1
            s2_ref[j] = s2
        return carry

    lax.fori_loop(0, nj, plane, 0)


def fixed_plane(j, ps_ref, h_ref, fk_ref, first):
    ni = ps_ref.shape[1]
    flow = fk_ref[j, pl.ds(7 - first, ni, stride=SUB), :]
    gain = RATE - flow if first == 0 else RATE + flow
    return ps_ref[j] + gain * h_ref[j]


def fix_body(core_ref, ps_ref, fk_ref, h_ref, af_ref, d_ref, as_ref, row_out, lo_out, hi_out, *, first):
    nj, rows, _ = d_ref.shape
    ni = rows // SUB
    other = 7 - first
    level = lax.broadcasted_iota(jnp.int32, (SUB, 128), 0)

    def some(j, carry):
        as_ref[j] = fixed_plane(j, ps_ref, h_ref, fk_ref, first)
        for dst, i in ((lo_out, 0), (hi_out, ni - 1)):
            v = jnp.where(level == first, af_ref[j, pl.ds(i, 1), :], d_ref[j, pl.ds(i * SUB, SUB), :])
            dst[j] = jnp.where(level == other, as_ref[j, pl.ds(i, 1), :], v)
        return carry

    lax.fori_loop(0, nj, some, 0)
    edge = (1 - core_ref[0]) * (nj - 1)
    row_out[...] = d_ref[edge]
    row_out[pl.ds(first, ni, stride=SUB), :] = af_ref[edge]
    row_out[pl.ds(other, ni, stride=SUB), :] = as_ref[edge]


def sums_body(core_ref, d_ref, ps_ref, fk_ref, h_ref, mid_ref, s1_ref, s2_ref, end_ref, v_ref, *, first):
    def some(j, carry):
        exact = fixed_plane(j, ps_ref, h_ref, fk_ref, first)
        end_ref[j, pl.ds(7 - first, ps_ref.shape[1], stride=SUB), :] = exact
        moved = exact - mid_ref[j]
        s1 = s1_ref[j] + moved
        s2 = s2_ref[j] + moved * moved
        v_ref[j, 0] = mid_ref[j] + s1 * (1.0 / SUB)
        v_ref[j, 1] = s2 - s1 * s1 * (1.0 / SUB)
        return carry

    lax.fori_loop(0, ps_ref.shape[0], some, 0)


def finish_body(d_ref, v_ref, anomaly_ref, end_ref, made, sent, sent_end):
    nj = d_ref.shape[0]
    ni = v_ref.shape[2]
    unroll = 8
    whole = pltpu.make_async_copy(d_ref, end_ref, sent_end)
    whole.start()

    def plane(j, carry):
        def some(n, inner):
            for m in range(unroll):
                i = n * unroll + m
                at = pl.multiple_of(i * SUB, SUB)
                mean = v_ref[j, 0, pl.ds(i, 1), :]
                scale = v_ref[j, 1, pl.ds(i, 1), :]
                made[j, pl.ds(at, SUB), :] = (d_ref[j, pl.ds(at, SUB), :] - mean) * scale
            return inner

        lax.fori_loop(0, ni // unroll, some, 0)
        pltpu.make_async_copy(made.at[j], anomaly_ref.at[j], sent).start()
        return carry

    lax.fori_loop(0, nj, plane, 0)
    pltpu.make_async_copy(made, anomaly_ref, sent).wait()
    whole.wait()


def finish_call(d, v):
    hbm = pl.BlockSpec(memory_space=pltpu.HBM)
    return pl.pallas_call(
        finish_body,
        in_specs=[pl.BlockSpec(memory_space=pltpu.VMEM)] * 2,
        out_specs=[hbm, hbm],
        out_shape=[jax.ShapeDtypeStruct(d.shape, d.dtype)] * 2,
        scratch_shapes=[pltpu.VMEM(d.shape, d.dtype), pltpu.SemaphoreType.DMA, pltpu.SemaphoreType.DMA],
        compiler_params=pltpu.CompilerParams(vmem_limit_bytes=10 << 20),
        name="finish",
    )(*in_vmem(d, v))


def send(value, axis, direction):
    size = lax.axis_size(axis)
    up = [(i, i + 1) for i in range(size - 1)]
    return lax.ppermute(value, axis, up if direction > 0 else [(b, a) for a, b in up])


def body(density, flow_j, flow_i, flow_k):
    nj, ni, nk, lanes = density.shape
    flat = lambda v: v.reshape(nj, ni * nk, lanes)
    core = lax.axis_index("rows").astype(jnp.int32).reshape(1)
    slabs = lax.axis_size("slabs")
    d, fj, fi, fk = flat(density), flat(flow_j), flat(flow_i), flat(flow_k)
    cube, square, line = d.shape, (nj, ni, lanes), (nj, SUB, lanes)
    edges = [cube[1:], line, line]
    ring = [pltpu.VMEM((3 * (cube[1] + 2 * SUB), lanes), jnp.float32)]
    plane_0, plane_7, row_send, lo_send, hi_send = local_call(prep_body, [square, square, *edges], core, d)
    planes = {0: plane_0, 7: plane_7}
    halo = {}
    for t in range(STEPS):
        first = 7 if t % 2 == 0 else 0
        other = 7 - first
        last = t == STEPS - 1
        if t == 0:
            halo[first] = send(planes[other], "slabs", -1)
        row = lax.ppermute(row_send, "rows", [(0, 1), (1, 0)])
        hi = send(lo_send, "cols", -1)
        lo = send(hi_send, "cols", 1)
        halo[other] = send(planes[first], "slabs", -1 if first == 0 else 1)
        if t == 0:
            fj, fi, fk = fetch_call(fj, fi, fk)
        d, exact, part, *sums = local_call(
            functools.partial(step_body, first=first, last=last),
            [cube] + [square] * (5 if last else 2),
            core,
            *(d, planes[0], planes[7], halo[first], row, lo, hi, fj, fi, fk),
            scratch=ring,
        )
        if last:
            break
        early = send(exact, "slabs", -1 if first == 0 else 1)
        fixed, row_send, lo_send, hi_send = local_call(
            functools.partial(fix_body, first=first), [square, *edges], core, *(part, fk, halo[other], exact, d)
        )
        planes = {first: exact, other: fixed}
        halo = {other: early}
    end, v = local_call(
        functools.partial(sums_body, first=first),
        [cube, (nj, 2, ni, lanes)],
        core,
        *(d, part, fk, halo[other], *sums),
        aliases={1: 0},
    )
    got = lax.all_to_all(v, "slabs", 0, 0, tiled=True)
    got = got.reshape(slabs, nj // slabs, 2, ni, lanes)
    mean = jnp.sum(got[:, :, 0], axis=0) / slabs
    off = got[:, :, 0] - mean
    line_variance = jnp.sum(got[:, :, 1] + nk * (off * off), axis=0) / (nk * slabs)
    mine = jnp.stack([mean, lax.rsqrt(line_variance + 0.0001)], axis=1)
    copies = jnp.broadcast_to(mine[None], (slabs, *mine.shape))
    v = lax.all_to_all(copies, "slabs", 0, 0, tiled=True).reshape(nj, 2, ni, lanes)
    anomaly, end = finish_call(end, v)
    return (anomaly.reshape(density.shape), end.reshape(density.shape))


def solution(mesh):
    placed = P("rows", "cols", "slabs", None)
    return jax.shard_map(
        body,
        mesh=mesh,
        in_specs=(placed,) * 4,
        out_specs=(placed, placed),
        check_vma=False,
    )
```

```python
import functools

import jax
import jax.numpy as jnp
from jax import lax
from jax.experimental import pallas as pl
from jax.experimental.pallas import tpu as pltpu
from jax.sharding import PartitionSpec as P

STEPS = 6
RATE = 0.05
SUB = 8


def in_vmem(*values):
    return [pltpu.with_memory_space_constraint(v, pltpu.VMEM) for v in values]


def local_call(body, outs, core, *values, scratch=(), aliases={}, stored=()):
    spec = pl.BlockSpec(memory_space=pltpu.VMEM)
    hbm = pl.BlockSpec(memory_space=pltpu.HBM)
    return pl.pallas_call(
        body,
        in_specs=[pl.BlockSpec(memory_space=pltpu.SMEM)] + [spec] * len(values),
        out_specs=[spec] * len(outs) + [hbm] * len(stored),
        out_shape=[pltpu.VMEM(shape, jnp.float32) for shape in outs]
        + [jax.ShapeDtypeStruct(shape, jnp.float32) for shape in stored],
        scratch_shapes=list(scratch),
        input_output_aliases=aliases,
        compiler_params=pltpu.CompilerParams(vmem_limit_bytes=4 << 20),
    )(core, *in_vmem(*values))


def fetch_body(*refs):
    count = len(refs) // 3
    copies = [pltpu.make_async_copy(refs[n], refs[count + n], refs[2 * count + n]) for n in range(count)]
    for copy in copies:
        copy.start()
    for copy in copies:
        copy.wait()


def fetch_call(*values):
    return pl.pallas_call(
        fetch_body,
        in_specs=[pl.BlockSpec(memory_space=pltpu.HBM)] * len(values),
        out_specs=[pl.BlockSpec(memory_space=pltpu.VMEM)] * len(values),
        out_shape=[pltpu.VMEM(v.shape, v.dtype) for v in values],
        scratch_shapes=[pltpu.SemaphoreType.DMA] * len(values),
        compiler_params=pltpu.CompilerParams(vmem_limit_bytes=4 << 20),
        name="fetch",
    )(*[pltpu.with_memory_space_constraint(v, pltpu.HBM) for v in values])


def prep_body(core_ref, d_ref, *refs, parts):
    outs, sems = refs[: len(parts)], refs[len(parts) :]
    nj, ni, _, _ = d_ref.shape
    edge = (1 - core_ref[0]) * (nj - 1)
    source = {
        0: lambda: d_ref.at[:, :, 0, :],
        7: lambda: d_ref.at[:, :, 7, :],
        "row": lambda: d_ref.at[edge],
        "low": lambda: d_ref.at[:, 0],
        "high": lambda: d_ref.at[:, ni - 1],
    }
    copies = [pltpu.make_async_copy(source[p](), o, s) for p, o, s in zip(parts, outs, sems)]
    for copy in copies:
        copy.start()
    for copy in copies:
        copy.wait()


def prep_call(core, density, *parts):
    nj, ni, nk, lanes = density.shape
    shape = {0: (nj, ni, lanes), 7: (nj, ni, lanes), "row": (ni, nk, lanes), "low": (nj, nk, lanes), "high": (nj, nk, lanes)}
    return pl.pallas_call(
        functools.partial(prep_body, parts=parts),
        in_specs=[pl.BlockSpec(memory_space=pltpu.SMEM), pl.BlockSpec(memory_space=pltpu.HBM)],
        out_specs=[pl.BlockSpec(memory_space=pltpu.VMEM)] * len(parts),
        out_shape=[pltpu.VMEM(shape[p], density.dtype) for p in parts],
        scratch_shapes=[pltpu.SemaphoreType.DMA] * len(parts),
        compiler_params=pltpu.CompilerParams(vmem_limit_bytes=4 << 20),
        name="prep",
    )(core, pltpu.with_memory_space_constraint(density, pltpu.HBM))


def step_body(core_ref, d_ref, a0_ref, a7_ref, h_ref, row_ref, lo_ref, hi_ref, fj_ref, fi_ref, fk_ref, *rest, first, last):
    if last:
        out_ref, af_ref, ps_ref, mid_ref, s1_ref, s2_ref, end_ref, ring, sent = rest
    else:
        out_ref, af_ref, ps_ref, ring = rest
    nj, rows, _ = d_ref.shape
    ni = rows // SUB
    pitch = rows + 2 * SUB
    other = 7 - first
    core = core_ref[0]
    level = lax.broadcasted_iota(jnp.int32, (SUB, 128), 0)

    def load(j):
        at = pl.multiple_of(lax.rem(j, 3) * pitch, SUB)
        ring[pl.ds(at + SUB, rows), :] = d_ref[j]
        ring[pl.ds(at + SUB, ni, stride=SUB), :] = a0_ref[j]
        ring[pl.ds(at + SUB + 7, ni, stride=SUB), :] = a7_ref[j]
        ring[pl.ds(at, SUB), :] = lo_ref[j]
        ring[pl.ds(at + SUB + rows, SUB), :] = hi_ref[j]

    ring[pl.ds(2 * pitch + SUB, rows), :] = jnp.where(core == 1, row_ref[...], 0.0)
    load(0)

    def plane(j, carry):
        here = lax.rem(j + 1, 3) * pitch
        middle = lax.rem(j, 3) * pitch
        below = lax.rem(j + 2, 3) * pitch

        @pl.when(j + 1 < nj)
        def _():
            load(j + 1)

        @pl.when(j + 1 == nj)
        def _():
            ring[pl.ds(pl.multiple_of(here + SUB, SUB), rows), :] = jnp.where(core == 0, row_ref[...], 0.0)

        unroll = 8

        def some(n, inner):
            base = pl.multiple_of(n * (unroll * SUB), SUB)
            for m in range(unroll):
                at = base + m * SUB
                mid = pl.multiple_of(middle + SUB + at, SUB)
                c = ring[pl.ds(mid, SUB), :]
                i_lo = ring[pl.ds(mid - SUB, SUB), :]
                i_hi = ring[pl.ds(mid + SUB, SUB), :]
                j_lo = ring[pl.ds(pl.multiple_of(below + SUB + at, SUB), SUB), :]
                j_hi = ring[pl.ds(pl.multiple_of(here + SUB + at, SUB), SUB), :]
                k_lo = jnp.where(level == 0, 0.0, pltpu.roll(c, 1, 0))
                k_hi = jnp.where(level == 7, 0.0, pltpu.roll(c, 7, 0))
                total = (j_lo + j_hi) + (i_lo + i_hi) + (k_lo + k_hi)
                new = (1.0 - 6.0 * RATE) * c + RATE * total
                new = new - fj_ref[j, pl.ds(at, SUB), :] * (j_hi - j_lo)
                new = new - fi_ref[j, pl.ds(at, SUB), :] * (i_hi - i_lo)
                new = new - fk_ref[j, pl.ds(at, SUB), :] * (k_hi - k_lo)
                out_ref[j, pl.ds(at, SUB), :] = new
            return inner

        lax.fori_loop(0, ni // unroll, some, 0)
        flow = fk_ref[j, pl.ds(first, ni, stride=SUB), :]
        gain = RATE + flow if first == 0 else RATE - flow
        exact = out_ref[j, pl.ds(first, ni, stride=SUB), :] + gain * h_ref[j]
        af_ref[j] = exact
        ps_ref[j] = out_ref[j, pl.ds(other, ni, stride=SUB), :]
        if last:
            out_ref[j, pl.ds(first, ni, stride=SUB), :] = exact
            centre = out_ref[j, pl.ds(3, ni, stride=SUB), :]
            moved = exact - centre
            s1 = moved
            s2 = moved * moved
            for k in (1, 2, 4, 5, 6):
                moved = out_ref[j, pl.ds(k, ni, stride=SUB), :] - centre
                s1 = s1 + moved
                s2 = s2 + moved * moved
            mid_ref[j] = centre
            s1_ref[j] = s1
            s2_ref[j] = s2
            pltpu.make_async_copy(out_ref.at[j], end_ref.at[j], sent).start()
        return carry

    lax.fori_loop(0, nj, plane, 0)
    if last:
        pltpu.make_async_copy(out_ref, end_ref, sent).wait()


def fixed_plane(j, ps_ref, h_ref, fk_ref, first):
    ni = ps_ref.shape[1]
    flow = fk_ref[j, pl.ds(7 - first, ni, stride=SUB), :]
    gain = RATE - flow if first == 0 else RATE + flow
    return ps_ref[j] + gain * h_ref[j]


def fix_body(core_ref, ps_ref, fk_ref, h_ref, af_ref, d_ref, as_ref, row_out, lo_out, hi_out, *, first):
    nj, rows, _ = d_ref.shape
    ni = rows // SUB
    other = 7 - first
    level = lax.broadcasted_iota(jnp.int32, (SUB, 128), 0)

    def some(j, carry):
        as_ref[j] = fixed_plane(j, ps_ref, h_ref, fk_ref, first)
        for dst, i in ((lo_out, 0), (hi_out, ni - 1)):
            v = jnp.where(level == first, af_ref[j, pl.ds(i, 1), :], d_ref[j, pl.ds(i * SUB, SUB), :])
            dst[j] = jnp.where(level == other, as_ref[j, pl.ds(i, 1), :], v)
        return carry

    lax.fori_loop(0, nj, some, 0)
    edge = (1 - core_ref[0]) * (nj - 1)
    row_out[...] = d_ref[edge]
    row_out[pl.ds(first, ni, stride=SUB), :] = af_ref[edge]
    row_out[pl.ds(other, ni, stride=SUB), :] = as_ref[edge]


def sums_body(core_ref, d_ref, ps_ref, fk_ref, h_ref, mid_ref, s1_ref, s2_ref, full_ref, as_ref, v_ref, *, first):
    def some(j, carry):
        exact = fixed_plane(j, ps_ref, h_ref, fk_ref, first)
        as_ref[j] = exact
        full_ref[j, pl.ds(7 - first, ps_ref.shape[1], stride=SUB), :] = exact
        moved = exact - mid_ref[j]
        s1 = s1_ref[j] + moved
        s2 = s2_ref[j] + moved * moved
        v_ref[j, 0] = mid_ref[j] + s1 * (1.0 / SUB)
        v_ref[j, 1] = s2 - s1 * s1 * (1.0 / SUB)
        return carry

    lax.fori_loop(0, ps_ref.shape[0], some, 0)


def finish_body(d_ref, as_ref, v_ref, _, anomaly_ref, end_ref, made, sent, sent_end, *, other):
    nj = d_ref.shape[0]
    ni = v_ref.shape[2]
    unroll = 8
    patch = pltpu.make_async_copy(as_ref, end_ref.at[:, :, other, :], sent_end)
    patch.start()

    def plane(j, carry):
        def some(n, inner):
            for m in range(unroll):
                i = n * unroll + m
                at = pl.multiple_of(i * SUB, SUB)
                mean = v_ref[j, 0, pl.ds(i, 1), :]
                scale = v_ref[j, 1, pl.ds(i, 1), :]
                made[j, pl.ds(at, SUB), :] = (d_ref[j, pl.ds(at, SUB), :] - mean) * scale
            return inner

        lax.fori_loop(0, ni // unroll, some, 0)
        pltpu.make_async_copy(made.at[j], anomaly_ref.at[j], sent).start()
        return carry

    lax.fori_loop(0, nj, plane, 0)
    pltpu.make_async_copy(made, anomaly_ref, sent).wait()
    patch.wait()


def finish_call(d, fixed, v, end, other):
    hbm = pl.BlockSpec(memory_space=pltpu.HBM)
    vmem = pl.BlockSpec(memory_space=pltpu.VMEM)
    return pl.pallas_call(
        functools.partial(finish_body, other=other),
        in_specs=[vmem, vmem, vmem, hbm],
        out_specs=[hbm, hbm],
        out_shape=[jax.ShapeDtypeStruct(d.shape, d.dtype), jax.ShapeDtypeStruct(end.shape, d.dtype)],
        scratch_shapes=[pltpu.VMEM(d.shape, d.dtype), pltpu.SemaphoreType.DMA, pltpu.SemaphoreType.DMA],
        input_output_aliases={3: 1},
        compiler_params=pltpu.CompilerParams(vmem_limit_bytes=10 << 20),
        name="finish",
    )(*in_vmem(d, fixed, v), end)


def send(value, axis, direction):
    size = lax.axis_size(axis)
    up = [(i, i + 1) for i in range(size - 1)]
    return lax.ppermute(value, axis, up if direction > 0 else [(b, a) for a, b in up])


def body(density, flow_j, flow_i, flow_k):
    nj, ni, nk, lanes = density.shape
    flat = lambda v: v.reshape(nj, ni * nk, lanes)
    core = lax.axis_index("rows").astype(jnp.int32).reshape(1)
    slabs = lax.axis_size("slabs")
    d, fj, fi, fk = flat(density), flat(flow_j), flat(flow_i), flat(flow_k)
    cube, square, line = d.shape, (nj, ni, lanes), (nj, SUB, lanes)
    edges = [cube[1:], line, line]
    ring = [pltpu.VMEM((3 * (cube[1] + 2 * SUB), lanes), jnp.float32)]
    (plane_0,) = prep_call(core, density, 0)
    plane_7, row_send, lo_send, hi_send = prep_call(core, density, 7, "row", "low", "high")
    row_send = row_send.reshape(ni * nk, lanes)
    planes = {0: plane_0, 7: plane_7}
    halo = {}
    for t in range(STEPS):
        first = 7 if t % 2 == 0 else 0
        other = 7 - first
        last = t == STEPS - 1
        if t == 0:
            halo[first] = send(planes[other], "slabs", -1)
        row = lax.ppermute(row_send, "rows", [(0, 1), (1, 0)])
        hi = send(lo_send, "cols", -1)
        lo = send(hi_send, "cols", 1)
        halo[other] = send(planes[first], "slabs", -1 if first == 0 else 1)
        if t == 0:
            fj, fi, fk = fetch_call(fj, fi, fk)
        d, exact, part, *sums = local_call(
            functools.partial(step_body, first=first, last=last),
            [cube] + [square] * (5 if last else 2),
            core,
            *(d, planes[0], planes[7], halo[first], row, lo, hi, fj, fi, fk),
            scratch=ring + [pltpu.SemaphoreType.DMA] * last,
            stored=[cube] * last,
        )
        if last:
            break
        early = send(exact, "slabs", -1 if first == 0 else 1)
        fixed, row_send, lo_send, hi_send = local_call(
            functools.partial(fix_body, first=first), [square, *edges], core, *(part, fk, halo[other], exact, d)
        )
        planes = {first: exact, other: fixed}
        halo = {other: early}
    *sums, end = sums
    full, fixed, v = local_call(
        functools.partial(sums_body, first=first),
        [cube, square, (nj, 2, ni, lanes)],
        core,
        *(d, part, fk, halo[other], *sums),
        aliases={1: 0},
    )
    got = lax.all_to_all(v, "slabs", 0, 0, tiled=True)
    got = got.reshape(slabs, nj // slabs, 2, ni, lanes)
    mean = jnp.sum(got[:, :, 0], axis=0) / slabs
    off = got[:, :, 0] - mean
    line_variance = jnp.sum(got[:, :, 1] + nk * (off * off), axis=0) / (nk * slabs)
    mine = jnp.stack([mean, lax.rsqrt(line_variance + 0.0001)], axis=1)
    copies = jnp.broadcast_to(mine[None], (slabs, *mine.shape))
    v = lax.all_to_all(copies, "slabs", 0, 0, tiled=True).reshape(nj, 2, ni, lanes)
    anomaly, end = finish_call(full, fixed, v, end.reshape(density.shape), other)
    return (anomaly.reshape(density.shape), end.reshape(density.shape))


def solution(mesh):
    placed = P("rows", "cols", "slabs", None)
    return jax.shard_map(
        body,
        mesh=mesh,
        in_specs=(placed,) * 4,
        out_specs=(placed, placed),
        check_vma=False,
    )
```
